128 devices in a mesh: tp: 4 (over x_hi, core), grp: 32 (over z, x_lo, y).
Axes of the slice: x: 4 (x_hi: 2, x_lo: 2; x = x_hi * 2 + x_lo), y: 4, z: 4, core: 2. Of those that a mesh axis runs over, the one named last changes fastest.
Arguments:
- flat_shards: bfloat16 [2, 2, 8448, 24576], P(None, None, ('grp', 'tp')), may hold values from -0.0625 to 0.0625
- offsets: int32 [2, 2], replicated, may hold values from 0 to 2
- probes: bfloat16 [512, 8192], P(None, 'grp'), may hold values from -6 to 6
Outputs:
- serving_tiles: bfloat16 [2, 2, 8192, 24576], P(None, None, 'grp', 'tp')
- hidden_check: bfloat16 [2, 512, 24576], P(None, 'grp', 'tp')
The draws below stay inside these ranges and needn't reach their ends.
All inputs are finite; a program needn't handle non-finite values.
Results may differ from the reference program's by a relative error of at most 0.001.
Values may be sent and summed in bfloat16 or wider, within the bound.
A program may use at most 320 MiB of HBM per device.

```python
import jax
import jax.numpy as jnp
from jax import lax

D = 8192
FF = 24576
LAYERS = 2
PAD = 2
PROBES = 512
ROWS_DEV = 64
N_GRP = 32
DEVICES = 128


def place_ends(result, rng, least, largest):
    longest = result.shape.index(max(result.shape))
    spots = []
    for shift in (0, 1):
        where = [jax.random.randint(jax.random.fold_in(rng, axis), (), 0, length) for axis, length in enumerate(result.shape)]
        where[longest] = (where[longest] + shift) % result.shape[longest]
        spots.append(tuple(where))
    return result.at[spots[0]].set(least).at[spots[1]].set(largest)


def level_of(key, extent, cuts, low, high):
    loudness, own = 1.0, jax.random.fold_in(key, 6)
    for axis_at, blocks in cuts:
        heights = jnp.exp(jax.random.uniform(jax.random.fold_in(own, axis_at), (blocks,), jnp.float32, low / len(cuts), high / len(cuts)))
        loudness = loudness * jnp.repeat(heights, extent[axis_at] // blocks).reshape([-1 if axis == axis_at else 1 for axis in range(len(extent))])
    return loudness


def bell_draw(key, shape, width, most, split=(), dtype=jnp.bfloat16):
    entries = jax.random.normal(key, shape, jnp.float32) * width
    if len(split) > 0:
        entries = level_of(key, shape, split, -0.22, 0.18) * entries
    return jnp.clip(entries, min=-most, max=most).astype(dtype)


def setup_inputs(seed: int = 0) -> dict:
    arg_keys = jax.random.split(jax.random.key(seed), 4)
    flat_shards = bell_draw(arg_keys[0], (LAYERS, 2, DEVICES * (ROWS_DEV + PAD), FF), D ** -0.5, 0.0625, ((2, 128),))
    offsets = place_ends(jax.random.randint(arg_keys[1], (LAYERS, 2), 0, PAD + 1), jax.random.fold_in(arg_keys[1], 1), 0, PAD).astype(jnp.int32)
    probes = bell_draw(arg_keys[2], (PROBES, D), 1.0, 6.0, ((1, 32),))
    return {"flat_shards": flat_shards, "offsets": offsets, "probes": probes}


def checksum(probes, tile):
    block = D // N_GRP

    def add_block(index, total):
        start = (index * block).astype(jnp.int32)
        rows = lax.dynamic_slice_in_dim(probes, start, block, 1)
        part = lax.dynamic_slice_in_dim(tile, start, block, 0)
        term = jnp.dot(rows, part, preferred_element_type=jnp.float32)
        return total + term

    empty = jnp.zeros((probes.shape[0], tile.shape[1]), jnp.float32)
    return lax.fori_loop(jnp.int32(0), jnp.int32(N_GRP), add_block, empty)


def reference(flat_shards, offsets, probes):
    layer_list = []
    check_list = []
    for which_layer in range(LAYERS):
        tensor_list = []
        for which_tensor in range(2):
            blocks = flat_shards[which_layer, which_tensor].reshape(DEVICES, ROWS_DEV + PAD, FF)
            start = offsets[which_layer, which_tensor].astype(jnp.int32)
            picked = lax.dynamic_slice_in_dim(blocks, start, ROWS_DEV, 1)
            tensor_list.append(picked.reshape(D, FF))
        gate_sums = checksum(probes, tensor_list[0])
        up_sums = checksum(probes, tensor_list[1])
        check_list.append((jax.nn.silu(gate_sums) * up_sums).astype(jnp.bfloat16))
        layer_list.append(jnp.stack(tensor_list))
    return jnp.stack(layer_list), jnp.stack(check_list)
```

```python
import functools

import jax
import jax.numpy as jnp
from jax import lax
from jax.experimental import pallas as pl
from jax.experimental.pallas import tpu as pltpu
from jax.sharding import PartitionSpec as P

PAD = 2
LANES = 128
N_Y = 4
N_Z = 4
N_Q = N_Y * N_Z
STAGES = 4
MESH = pl.DeviceIdType.MESH

STEPS = (
    (2, 2), (1, 0), (0, 1), (3, 0), (0, 3), (2, 1), (1, 2), (2, 3),
    (3, 2), (1, 1), (3, 3), (2, 0), (0, 2), (1, 3), (3, 1),
)


def kernel(
    layers, flat, offsets, probes, tiles_out, check_out,
    stage, wide, to_tp, tile, column, features, total, other, gated, check,
    stage_sem, send_a, recv_a, send_b, recv_b, own_p, send_p, recv_p, send_f, recv_f,
    send_r, recv_r, send_h, recv_h, out_sem,
):
    tp = lax.axis_index("tp")
    grp = lax.axis_index("grp")
    core = lax.rem(tp, 2)
    z, x_lo, y = grp // 8, lax.rem(grp // 4, 2), lax.rem(grp, 4)
    mine = z * N_Y + y
    rows = to_tp.shape[4]
    blocks = to_tp.shape[3]
    chunks = tile.shape[0]
    per_layer = chunks // layers
    width = blocks * LANES
    tile_cols = per_layer * width
    tile_rows = tile.shape[3]
    half = other.shape[1]
    each = half // N_Q

    def peer(dz, dy):
        z2, y2 = lax.rem(z + dz, N_Z), lax.rem(y + dy, N_Y)
        return z2 * N_Y + y2, {"grp": z2 * 8 + x_lo * 4 + y2}

    def remote(src, dst, send, recv, where):
        return pltpu.make_async_remote_copy(
            src_ref=src, dst_ref=dst, send_sem=send, recv_sem=recv,
            device_id=where, device_id_type=MESH,
        )

    def drained(ref, sem):
        pltpu.make_async_copy(ref, ref, sem).wait()

    units = chunks * 2 * 4

    def unit_of(u):
        chunk, tensor, step = u // 8, lax.rem(u // 4, 2), lax.rem(u, 4)
        return chunk, tensor, step, lax.rem(tp + step + 1, 4)

    def fetch(u):
        chunk, tensor, step, dest = unit_of(u)
        start = dest * tile_cols + lax.rem(chunk, per_layer) * width
        slot = lax.rem(u, STAGES)
        return pltpu.make_async_copy(
            flat.at[chunk // per_layer, tensor, :, pl.ds(pl.multiple_of(start, LANES), width)],
            stage.at[slot], stage_sem.at[slot],
        )

    for u in range(STAGES):
        fetch(u).start()

    group = N_Y * each
    own = [
        pltpu.make_async_copy(
            probes.at[pl.ds((at * 2 + lo) * group, group)],
            features.at[mine, pl.ds(lo * half + at * group, group)],
            own_p.at[at * 2 + lo],
        )
        for at in range(N_Z) for lo in range(2)
    ]
    for copy in own:
        copy.start()
    for copy in own:
        copy.wait()
    share = pl.ds(pl.multiple_of(core * half, half), half)
    for dz, dy in STEPS:
        _, where = peer(dz, dy)
        remote(features.at[mine, share], features.at[mine, share], send_p, recv_p, where).start()

    def pick(u, _):
        chunk, tensor, step, dest = unit_of(u)
        slot = lax.rem(u, STAGES)
        fetch(u).wait()
        for block in range(blocks):
            wide[block] = stage[slot, :, block * LANES:(block + 1) * LANES].astype(jnp.float32)
        first = offsets[chunk // per_layer, tensor]

        @pl.when(step < 3)
        def _():
            for block in range(blocks):
                to_tp[chunk, tensor, step, block] = wide[
                    block, pl.ds(first, rows)
                ].astype(jnp.bfloat16)
            remote(
                to_tp.at[chunk, tensor, step],
                tile.at[chunk, :, tensor, pl.ds(pl.multiple_of(tp * rows, rows), rows)],
                send_a, recv_a.at[chunk], {"tp": dest},
            ).start()

        @pl.when(step == 3)
        def _():
            for block in range(blocks):
                tile[chunk, block, tensor, pl.ds(pl.multiple_of(tp * rows, rows), rows)] = wide[
                    block, pl.ds(first, rows)
                ].astype(jnp.bfloat16)

        @pl.when(u + STAGES < units)
        def _():
            fetch(u + STAGES).start()

        return 0

    lax.fori_loop(0, units, pick, 0)

    others = features.at[pl.ds(0, N_Q - 1), pl.ds(0, half)]
    drained(others, recv_p)
    neighbour = {"tp": tp + 1 - 2 * core}

    def hand_on(step, _):
        at = lax.rem(mine + step + 1, N_Q)
        remote(features.at[at, share], features.at[at, share], send_f, recv_f, neighbour).start()
        return 0

    lax.fori_loop(0, N_Q - 1, hand_on, 0)
    drained(others, recv_f)

    def spread(chunk):
        drained(to_tp.at[0], recv_a.at[chunk])
        for dz, dy in STEPS:
            at, where = peer(dz, dy)
            remote(tile.at[chunk, at], column.at[chunk, mine], send_b, recv_b.at[chunk], where).start()
        column[chunk, mine] = tile[chunk, mine]
        layer, part = chunk // per_layer, lax.rem(chunk, per_layer)

        def put(block, _):
            start = pl.multiple_of(part * width + block * LANES, LANES)
            for tensor in range(2):
                pltpu.make_async_copy(
                    tile.at[chunk, block, tensor],
                    tiles_out.at[layer, tensor, :, pl.ds(start, LANES)],
                    out_sem,
                ).start()
            return 0

        lax.fori_loop(0, blocks, put, 0)

    partner = {"grp": grp + 4 - 8 * x_lo}
    keep = pl.ds(pl.multiple_of(x_lo * half, half), half)
    give = pl.ds(pl.multiple_of((1 - x_lo) * half, half), half)

    def multiply(chunk):
        drained(column.at[chunk, pl.ds(0, N_Q - 1)], recv_b.at[chunk])
        total[chunk] = jnp.zeros(total.shape[1:], jnp.float32)

        def add(at, _):
            weights = jnp.concatenate([column[chunk, at, 0], column[chunk, at, 1]], axis=1)
            total[chunk] += jnp.dot(features[at], weights, preferred_element_type=jnp.float32)
            return 0

        lax.fori_loop(0, N_Q, add, 0)
        remote(total.at[chunk, give], other.at[chunk], send_r, recv_r.at[chunk], partner).start()

    def gate(chunk, _):
        drained(other.at[chunk], recv_r.at[chunk])
        sums = total[chunk, keep] + other[chunk]
        v, up = sums[:, :LANES], sums[:, LANES:]
        hidden = (v / (1.0 + jnp.exp(-v)) * up).astype(jnp.bfloat16)
        gated[chunk] = hidden.reshape(N_Q, each, LANES)
        check[mine, chunk] = gated[chunk, mine]
        for dz, dy in STEPS:
            at, where = peer(dz, dy)
            remote(gated.at[chunk, at], check.at[mine, chunk], send_h, recv_h, where).start()
        return 0

    spread(0)

    def step(chunk, _):
        spread(chunk)
        multiply(chunk - 1)
        return 0

    lax.fori_loop(1, chunks, step, 0)
    multiply(chunks - 1)
    lax.fori_loop(0, chunks, gate, 0)

    arrived = check.at[pl.ds(0, N_Q - 1)]
    drained(arrived, recv_h)
    for chunk in range(chunks):
        for at in range(N_Q):
            start = (chunk % per_layer) * width + at * LANES
            check_out[chunk // per_layer, :, start:start + LANES] = check[at, chunk]

    drained(to_tp, send_a)
    drained(column.at[:, pl.ds(0, N_Q - 1)], send_b)
    drained(others, send_p)
    drained(others, send_f)
    drained(other, send_r)
    drained(arrived, send_h)
    drained(tile, out_sem)


def per_device(flat_shards, offsets, probes):
    tp_count = lax.axis_size("tp")
    layers = flat_shards.shape[0]
    rows = flat_shards.shape[2] - PAD
    tile_cols = flat_shards.shape[3] // tp_count
    tile_rows = rows * tp_count
    count = probes.shape[0]
    half = count // 2
    each = half // N_Q
    width = N_Q * LANES
    chunks = layers * (tile_cols // width)
    bf16, f32 = jnp.bfloat16, jnp.float32
    dma = pltpu.SemaphoreType.DMA
    return pl.pallas_call(
        functools.partial(kernel, layers),
        out_shape=(
            jax.ShapeDtypeStruct((layers, 2, tile_rows, tile_cols), bf16),
            jax.ShapeDtypeStruct((layers, each, tile_cols), bf16),
        ),
        in_specs=[
            pl.BlockSpec(memory_space=pl.ANY),
            pl.BlockSpec(memory_space=pltpu.SMEM),
            pl.BlockSpec(memory_space=pl.ANY),
        ],
        out_specs=(pl.BlockSpec(memory_space=pl.ANY), pl.BlockSpec(memory_space=pltpu.VMEM)),
        scratch_shapes=[
            pltpu.VMEM((STAGES, rows + PAD, width), bf16),
            pltpu.VMEM((N_Q, rows + PAD, LANES), f32),
            pltpu.VMEM((chunks, 2, 3, N_Q, rows, LANES), bf16),
            pltpu.VMEM((chunks, N_Q, 2, tile_rows, LANES), bf16),
            pltpu.VMEM((chunks, N_Q, 2, tile_rows, LANES), bf16),
            pltpu.VMEM((N_Q, count, probes.shape[1]), bf16),
            pltpu.VMEM((chunks, count, 2 * LANES), f32),
            pltpu.VMEM((chunks, half, 2 * LANES), f32),
            pltpu.VMEM((chunks, N_Q, each, LANES), bf16),
            pltpu.VMEM((N_Q, chunks, each, LANES), bf16),
            dma((STAGES,)), dma, dma((chunks,)), dma, dma((chunks,)),
            dma((2 * N_Z,)), dma, dma, dma, dma,
            dma, dma((chunks,)), dma, dma, dma,
        ],
        compiler_params=pltpu.CompilerParams(has_side_effects=True, vmem_limit_bytes=62 * 2**20),
        name="reshard_check",
    )(flat_shards, offsets, probes)


def solution(mesh):
    placed = (P(None, None, ("grp", "tp"), None), P(), P(None, "grp"))
    return jax.shard_map(
        per_device,
        mesh=mesh,
        in_specs=placed,
        out_specs=(P(None, None, "grp", "tp"), P(None, "grp", "tp")),
        check_vma=False,
    )
```

```python
import functools

import jax
import jax.numpy as jnp
from jax import lax
from jax.experimental import pallas as pl
from jax.experimental.pallas import tpu as pltpu
from jax.sharding import PartitionSpec as P

PAD = 2
LANES = 128
N_Y = 4
N_Z = 4
N_Q = N_Y * N_Z
STAGES = 4
LAG = 3
MESH = pl.DeviceIdType.MESH

STEPS = (
    (2, 2), (1, 0), (0, 1), (3, 0), (0, 3), (2, 1), (1, 2), (2, 3),
    (3, 2), (1, 1), (3, 3), (2, 0), (0, 2), (1, 3), (3, 1),
)


def kernel(
    layers, flat, offsets, probes, tiles_out, check_out,
    stage, wide, to_tp, tile, column, features, total, other, gated, check,
    stage_sem, send_a, recv_n, recv_a, send_b, recv_b, own_p, send_p, recv_p, send_f, recv_f,
    send_r, recv_r, send_h, recv_h, out_sem,
):
    tp = lax.axis_index("tp")
    grp = lax.axis_index("grp")
    core = lax.rem(tp, 2)
    z, x_lo, y = grp // 8, lax.rem(grp // 4, 2), lax.rem(grp, 4)
    mine = z * N_Y + y
    rows = to_tp.shape[4]
    blocks = to_tp.shape[3]
    chunks = tile.shape[0]
    per_layer = chunks // layers
    width = blocks * LANES
    tile_cols = per_layer * width
    pair = 2 * rows
    half = other.shape[1]
    each = half // N_Q

    def peer(dz, dy):
        z2, y2 = lax.rem(z + dz, N_Z), lax.rem(y + dy, N_Y)
        return z2 * N_Y + y2, {"grp": z2 * 8 + x_lo * 4 + y2}

    def remote(src, dst, send, recv, where):
        return pltpu.make_async_remote_copy(
            src_ref=src, dst_ref=dst, send_sem=send, recv_sem=recv,
            device_id=where, device_id_type=MESH,
        )

    def drained(ref, sem):
        pltpu.make_async_copy(ref, ref, sem).wait()

    units = chunks * 2 * 4

    def unit_of(u):
        chunk, tensor, step = u // 8, lax.rem(u // 4, 2), lax.rem(u, 4)
        far = 2 - 2 * (tp // 2) + lax.rem(core + step, 2)
        near = 2 * (tp // 2) + lax.rem(core + step + 1, 2)
        return chunk, tensor, step, jnp.where(step < 2, far, near)

    def fetch(u):
        chunk, tensor, step, dest = unit_of(u)
        start = dest * tile_cols + lax.rem(chunk, per_layer) * width
        slot = lax.rem(u, STAGES)
        return pltpu.make_async_copy(
            flat.at[chunk // per_layer, tensor, :, pl.ds(pl.multiple_of(start, LANES), width)],
            stage.at[slot], stage_sem.at[slot],
        )

    for u in range(STAGES):
        fetch(u).start()

    group = N_Y * each
    own = [
        pltpu.make_async_copy(
            probes.at[pl.ds((at * 2 + lo) * group, group)],
            features.at[mine, pl.ds(lo * half + at * group, group)],
            own_p.at[at * 2 + lo],
        )
        for at in range(N_Z) for lo in range(2)
    ]
    for copy in own:
        copy.start()
    for copy in own:
        copy.wait()
    share = pl.ds(pl.multiple_of(core * half, half), half)
    for dz, dy in STEPS:
        _, where = peer(dz, dy)
        remote(features.at[mine, share], features.at[mine, share], send_p, recv_p, where).start()

    def picked(block, first):
        return wide[block, pl.ds(first, rows)].astype(jnp.bfloat16)

    own_rows = pl.ds(pl.multiple_of(tp * rows, rows), rows)
    near_rows = pl.ds(pl.multiple_of((tp // 2) * pair, pair), pair)
    far_rows = pl.ds(pl.multiple_of((1 - tp // 2) * pair, pair), pair)

    def pick(u, _):
        chunk, tensor, step, dest = unit_of(u)
        slot = lax.rem(u, STAGES)
        fetch(u).wait()
        for block in range(blocks):
            wide[block] = stage[slot, :, block * LANES:(block + 1) * LANES].astype(jnp.float32)
        first = offsets[chunk // per_layer, tensor]

        def send(recv):
            for block in range(blocks):
                to_tp[chunk, tensor, step, block] = picked(block, first)
            remote(
                to_tp.at[chunk, tensor, step], tile.at[chunk, :, tensor, own_rows],
                send_a, recv.at[chunk], {"tp": dest},
            ).start()

        @pl.when(step < 2)
        def _():
            send(recv_a)

        @pl.when(step == 2)
        def _():
            send(recv_n)

        @pl.when(step == 3)
        def _():
            for block in range(blocks):
                tile[chunk, block, tensor, own_rows] = picked(block, first)

        @pl.when(u + STAGES < units)
        def _():
            fetch(u + STAGES).start()

        return 0

    def spread(chunk, which):
        for dz, dy in STEPS:
            at, where = peer(dz, dy)
            remote(
                tile.at[chunk, at, :, which], column.at[chunk, mine, :, which],
                send_b, recv_b.at[chunk], where,
            ).start()

    def spread_near(chunk):
        drained(to_tp.at[0, :, 0], recv_n.at[chunk])
        spread(chunk, near_rows)

    def picks(chunk, _):
        lax.fori_loop(chunk * 8, chunk * 8 + 8, pick, 0)

        @pl.when(chunk > 0)
        def _():
            spread_near(chunk - 1)

        return 0

    lax.fori_loop(0, chunks, picks, 0)
    spread_near(chunks - 1)

    others = features.at[pl.ds(0, N_Q - 1), pl.ds(0, half)]
    drained(others, recv_p)
    neighbour = {"tp": tp + 1 - 2 * core}

    def hand_on(step, _):
        at = lax.rem(mine + step + 1, N_Q)
        remote(features.at[at, share], features.at[at, share], send_f, recv_f, neighbour).start()
        return 0

    lax.fori_loop(0, N_Q - 1, hand_on, 0)
    drained(others, recv_f)

    def spread_far(chunk):
        drained(to_tp.at[0, :, pl.ds(0, 2)], recv_a.at[chunk])
        spread(chunk, far_rows)
        column[chunk, mine] = tile[chunk, mine]
        layer, part = chunk // per_layer, lax.rem(chunk, per_layer)

        def put(block, _):
            start = pl.multiple_of(part * width + block * LANES, LANES)
            for tensor in range(2):
                pltpu.make_async_copy(
                    tile.at[chunk, block, tensor],
                    tiles_out.at[layer, tensor, :, pl.ds(start, LANES)],
                    out_sem,
                ).start()
            return 0

        lax.fori_loop(0, blocks, put, 0)

    partner = {"grp": grp + 4 - 8 * x_lo}
    keep = pl.ds(pl.multiple_of(x_lo * half, half), half)
    give = pl.ds(pl.multiple_of((1 - x_lo) * half, half), half)

    def multiply(chunk):
        drained(column.at[chunk, pl.ds(0, N_Q - 1)], recv_b.at[chunk])
        total[chunk] = jnp.zeros(total.shape[1:], jnp.float32)

        def add(at, _):
            weights = jnp.concatenate([column[chunk, at, 0], column[chunk, at, 1]], axis=1)
            total[chunk] += jnp.dot(features[at], weights, preferred_element_type=jnp.float32)
            return 0

        lax.fori_loop(0, N_Q, add, 0)
        remote(total.at[chunk, give], other.at[chunk], send_r, recv_r.at[chunk], partner).start()

    def gate(chunk):
        drained(other.at[chunk], recv_r.at[chunk])
        sums = total[chunk, keep] + other[chunk]
        v, up = sums[:, :LANES], sums[:, LANES:]
        hidden = (v / (1.0 + jnp.exp(-v)) * up).astype(jnp.bfloat16)
        gated[chunk] = hidden.reshape(N_Q, each, LANES)
        check[mine, chunk] = gated[chunk, mine]
        for dz, dy in STEPS:
            at, where = peer(dz, dy)
            remote(gated.at[chunk, at], check.at[mine, chunk], send_h, recv_h, where).start()

    def step(chunk, _):
        spread_far(chunk)

        @pl.when(chunk >= LAG)
        def _():
            multiply(chunk - LAG)

        return 0

    def finish(chunk, _):
        multiply(chunk)
        gate(chunk - LAG)
        return 0

    lax.fori_loop(0, chunks, step, 0)
    lax.fori_loop(chunks - LAG, chunks, finish, 0)
    for chunk in range(chunks - LAG, chunks):
        gate(chunk)

    arrived = check.at[pl.ds(0, N_Q - 1)]
    drained(arrived, recv_h)
    for chunk in range(chunks):
        for at in range(N_Q):
            start = (chunk % per_layer) * width + at * LANES
            check_out[chunk // per_layer, :, start:start + LANES] = check[at, chunk]

    drained(to_tp, send_a)
    drained(column.at[:, pl.ds(0, N_Q - 1)], send_b)
    drained(others, send_p)
    drained(others, send_f)
    drained(other, send_r)
    drained(arrived, send_h)
    drained(tile, out_sem)


def per_device(flat_shards, offsets, probes):
    tp_count = lax.axis_size("tp")
    layers = flat_shards.shape[0]
    rows = flat_shards.shape[2] - PAD
    tile_cols = flat_shards.shape[3] // tp_count
    tile_rows = rows * tp_count
    count = probes.shape[0]
    half = count // 2
    each = half // N_Q
    width = N_Q * LANES
    chunks = layers * (tile_cols // width)
    bf16, f32 = jnp.bfloat16, jnp.float32
    dma = pltpu.SemaphoreType.DMA
    return pl.pallas_call(
        functools.partial(kernel, layers),
        out_shape=(
            jax.ShapeDtypeStruct((layers, 2, tile_rows, tile_cols), bf16),
            jax.ShapeDtypeStruct((layers, each, tile_cols), bf16),
        ),
        in_specs=[
            pl.BlockSpec(memory_space=pl.ANY),
            pl.BlockSpec(memory_space=pltpu.SMEM),
            pl.BlockSpec(memory_space=pl.ANY),
        ],
        out_specs=(pl.BlockSpec(memory_space=pl.ANY), pl.BlockSpec(memory_space=pltpu.VMEM)),
        scratch_shapes=[
            pltpu.VMEM((STAGES, rows + PAD, width), bf16),
            pltpu.VMEM((N_Q, rows + PAD, LANES), f32),
            pltpu.VMEM((chunks, 2, 3, N_Q, rows, LANES), bf16),
            pltpu.VMEM((chunks, N_Q, 2, tile_rows, LANES), bf16),
            pltpu.VMEM((chunks, N_Q, 2, tile_rows, LANES), bf16),
            pltpu.VMEM((N_Q, count, probes.shape[1]), bf16),
            pltpu.VMEM((chunks, count, 2 * LANES), f32),
            pltpu.VMEM((chunks, half, 2 * LANES), f32),
            pltpu.VMEM((chunks, N_Q, each, LANES), bf16),
            pltpu.VMEM((N_Q, chunks, each, LANES), bf16),
            dma((STAGES,)), dma, dma((chunks,)), dma((chunks,)), dma, dma((chunks,)),
            dma((2 * N_Z,)), dma, dma, dma, dma,
            dma, dma((chunks,)), dma, dma, dma,
        ],
        compiler_params=pltpu.CompilerParams(has_side_effects=True, vmem_limit_bytes=62 * 2**20),
        name="reshard_check",
    )(flat_shards, offsets, probes)


def solution(mesh):
    placed = (P(None, None, ("grp", "tp"), None), P(), P(None, "grp"))
    return jax.shard_map(
        per_device,
        mesh=mesh,
        in_specs=placed,
        out_specs=(P(None, None, "grp", "tp"), P(None, "grp", "tp")),
        check_vma=False,
    )
```

```python
import functools

import jax
import jax.numpy as jnp
from jax import lax
from jax.experimental import pallas as pl
from jax.experimental.pallas import tpu as pltpu
from jax.sharding import PartitionSpec as P

PAD = 2
LANES = 128
N_Y = 4
N_Z = 4
N_Q = N_Y * N_Z
STAGES = 4
LAG = 3
MESH = pl.DeviceIdType.MESH

STEPS = (
    (2, 2), (1, 0), (0, 1), (3, 0), (0, 3), (2, 1), (1, 2), (2, 3),
    (3, 2), (1, 1), (3, 3), (2, 0), (0, 2), (1, 3), (3, 1),
)


def kernel(
    layers, flat, offsets, probes, tiles_out, check_out,
    stage, to_tp, tile, column, features, total, other, gated, check,
    stage_sem, send_a, recv_n, recv_a, send_b, recv_b, own_p, send_p, recv_p, send_f, recv_f,
    send_r, recv_r, send_h, recv_h, out_sem,
):
    tp = lax.axis_index("tp")
    grp = lax.axis_index("grp")
    core = lax.rem(tp, 2)
    z, x_lo, y = grp // 8, lax.rem(grp // 4, 2), lax.rem(grp, 4)
    mine = z * N_Y + y
    rows = to_tp.shape[4]
    blocks = to_tp.shape[3]
    chunks = tile.shape[0]
    per_layer = chunks // layers
    width = blocks * LANES
    tile_cols = per_layer * width
    pair = 2 * rows
    half = other.shape[1]
    each = half // N_Q

    def peer(dz, dy):
        z2, y2 = lax.rem(z + dz, N_Z), lax.rem(y + dy, N_Y)
        return z2 * N_Y + y2, {"grp": z2 * 8 + x_lo * 4 + y2}

    def remote(src, dst, send, recv, where):
        return pltpu.make_async_remote_copy(
            src_ref=src, dst_ref=dst, send_sem=send, recv_sem=recv,
            device_id=where, device_id_type=MESH,
        )

    def drained(ref, sem):
        pltpu.make_async_copy(ref, ref, sem).wait()

    units = chunks * 4

    def unit_of(u):
        chunk, step = u // 4, lax.rem(u, 4)
        far = 2 - 2 * (tp // 2) + lax.rem(core + step, 2)
        near = 2 * (tp // 2) + lax.rem(core + step + 1, 2)
        return chunk, step, jnp.where(step < 2, far, near)

    def fetch(u):
        chunk, step, dest = unit_of(u)
        start = dest * tile_cols + lax.rem(chunk, per_layer) * width
        slot = lax.rem(u, STAGES)
        return pltpu.make_async_copy(
            flat.at[chunk // per_layer, :, :, pl.ds(pl.multiple_of(start, LANES), width)],
            stage.at[slot], stage_sem.at[slot],
        )

    for u in range(STAGES):
        fetch(u).start()

    group = N_Y * each
    own = [
        pltpu.make_async_copy(
            probes.at[pl.ds((at * 2 + lo) * group, group)],
            features.at[mine, pl.ds(lo * half + at * group, group)],
            own_p.at[at * 2 + lo],
        )
        for at in range(N_Z) for lo in range(2)
    ]
    for copy in own:
        copy.start()
    for copy in own:
        copy.wait()
    share = pl.ds(pl.multiple_of(core * half, half), half)
    for dz, dy in STEPS:
        _, where = peer(dz, dy)
        remote(features.at[mine, share], features.at[mine, share], send_p, recv_p, where).start()

    held = stage.shape[1]
    row = lax.broadcasted_iota(jnp.int32, (pair, 2 * held), 0)
    col = lax.broadcasted_iota(jnp.int32, (pair, 2 * held), 1)

    own_rows = pl.ds(pl.multiple_of(tp * rows, rows), rows)
    near_rows = pl.ds(pl.multiple_of((tp // 2) * pair, pair), pair)
    far_rows = pl.ds(pl.multiple_of((1 - tp // 2) * pair, pair), pair)

    def pick(u, _):
        chunk, step, dest = unit_of(u)
        slot = lax.rem(u, STAGES)
        fetch(u).wait()
        layer = chunk // per_layer
        wanted = jnp.where(row < rows, 2 * (row + offsets[layer, 0]), 2 * (row - rows + offsets[layer, 1]) + 1)
        chosen = jnp.where(col == wanted, 1.0, 0.0).astype(jnp.bfloat16)

        def picked(store):
            for at in range(0, blocks, 2):
                both = stage[slot, :, :, at * LANES:(at + 2) * LANES].reshape(2 * held, 2 * LANES)
                out = jnp.dot(chosen, both, preferred_element_type=jnp.float32).astype(jnp.bfloat16)
                for block in range(2):
                    for tensor in range(2):
                        store(at + block, tensor, out[
                            tensor * rows:(tensor + 1) * rows, block * LANES:(block + 1) * LANES
                        ])

        def send(recv):
            def store(block, tensor, value):
                to_tp[chunk, tensor, step, block] = value

            picked(store)
            for tensor in range(2):
                remote(
                    to_tp.at[chunk, tensor, step], tile.at[chunk, :, tensor, own_rows],
                    send_a, recv.at[chunk], {"tp": dest},
                ).start()

        @pl.when(step < 2)
        def _():
            send(recv_a)

        @pl.when(step == 2)
        def _():
            send(recv_n)

        @pl.when(step == 3)
        def _():
            def store(block, tensor, value):
                tile[chunk, block, tensor, own_rows] = value

            picked(store)

        @pl.when(u + STAGES < units)
        def _():
            fetch(u + STAGES).start()

        return 0

    def spread(chunk, which):
        for dz, dy in STEPS:
            at, where = peer(dz, dy)
            remote(
                tile.at[chunk, at, :, which], column.at[chunk, mine, :, which],
                send_b, recv_b.at[chunk], where,
            ).start()

    def spread_near(chunk):
        drained(to_tp.at[0, :, 0], recv_n.at[chunk])
        spread(chunk, near_rows)

    def picks(chunk, _):
        lax.fori_loop(chunk * 4, chunk * 4 + 4, pick, 0)

        @pl.when(chunk > 0)
        def _():
            spread_near(chunk - 1)

        return 0

    lax.fori_loop(0, chunks, picks, 0)
    spread_near(chunks - 1)

    others = features.at[pl.ds(0, N_Q - 1), pl.ds(0, half)]
    drained(others, recv_p)
    neighbour = {"tp": tp + 1 - 2 * core}

    def hand_on(step, _):
        at = lax.rem(mine + step + 1, N_Q)
        remote(features.at[at, share], features.at[at, share], send_f, recv_f, neighbour).start()
        return 0

    lax.fori_loop(0, N_Q - 1, hand_on, 0)
    drained(others, recv_f)

    def spread_far(chunk):
        drained(to_tp.at[0, :, pl.ds(0, 2)], recv_a.at[chunk])
        spread(chunk, far_rows)
        column[chunk, mine] = tile[chunk, mine]
        layer, part = chunk // per_layer, lax.rem(chunk, per_layer)

        def put(block, _):
            start = pl.multiple_of(part * width + block * LANES, LANES)
            for tensor in range(2):
                pltpu.make_async_copy(
                    tile.at[chunk, block, tensor],
                    tiles_out.at[layer, tensor, :, pl.ds(start, LANES)],
                    out_sem,
                ).start()
            return 0

        lax.fori_loop(0, blocks, put, 0)

    partner = {"grp": grp + 4 - 8 * x_lo}
    keep = pl.ds(pl.multiple_of(x_lo * half, half), half)
    give = pl.ds(pl.multiple_of((1 - x_lo) * half, half), half)

    def multiply(chunk):
        drained(column.at[chunk, pl.ds(0, N_Q - 1)], recv_b.at[chunk])
        total[chunk] = jnp.zeros(total.shape[1:], jnp.float32)

        def add(at, _):
            weights = jnp.concatenate([column[chunk, at, 0], column[chunk, at, 1]], axis=1)
            total[chunk] += jnp.dot(features[at], weights, preferred_element_type=jnp.float32)
            return 0

        lax.fori_loop(0, N_Q, add, 0)
        remote(total.at[chunk, give], other.at[chunk], send_r, recv_r.at[chunk], partner).start()

    def gate(chunk):
        drained(other.at[chunk], recv_r.at[chunk])
        sums = total[chunk, keep] + other[chunk]
        v, up = sums[:, :LANES], sums[:, LANES:]
        hidden = (v / (1.0 + jnp.exp(-v)) * up).astype(jnp.bfloat16)
        gated[chunk] = hidden.reshape(N_Q, each, LANES)
        check[mine, chunk] = gated[chunk, mine]
        for dz, dy in STEPS:
            at, where = peer(dz, dy)
            remote(gated.at[chunk, at], check.at[mine, chunk], send_h, recv_h, where).start()

    def step(chunk, _):
        spread_far(chunk)

        @pl.when(chunk >= LAG)
        def _():
            multiply(chunk - LAG)

        return 0

    def finish(chunk, _):
        multiply(chunk)
        gate(chunk - LAG)
        return 0

    lax.fori_loop(0, chunks, step, 0)
    lax.fori_loop(chunks - LAG, chunks, finish, 0)
    for chunk in range(chunks - LAG, chunks):
        gate(chunk)

    arrived = check.at[pl.ds(0, N_Q - 1)]
    drained(arrived, recv_h)
    for chunk in range(chunks):
        for at in range(N_Q):
            start = (chunk % per_layer) * width + at * LANES
            check_out[chunk // per_layer, :, start:start + LANES] = check[at, chunk]

    drained(to_tp, send_a)
    drained(column.at[:, pl.ds(0, N_Q - 1)], send_b)
    drained(others, send_p)
    drained(others, send_f)
    drained(other, send_r)
    drained(arrived, send_h)
    drained(tile, out_sem)


def per_device(flat_shards, offsets, probes):
    tp_count = lax.axis_size("tp")
    layers = flat_shards.shape[0]
    rows = flat_shards.shape[2] - PAD
    tile_cols = flat_shards.shape[3] // tp_count
    tile_rows = rows * tp_count
    count = probes.shape[0]
    half = count // 2
    each = half // N_Q
    width = N_Q * LANES
    chunks = layers * (tile_cols // width)
    bf16, f32 = jnp.bfloat16, jnp.float32
    dma = pltpu.SemaphoreType.DMA
    return pl.pallas_call(
        functools.partial(kernel, layers),
        out_shape=(
            jax.ShapeDtypeStruct((layers, 2, tile_rows, tile_cols), bf16),
            jax.ShapeDtypeStruct((layers, each, tile_cols), bf16),
        ),
        in_specs=[
            pl.BlockSpec(memory_space=pl.ANY),
            pl.BlockSpec(memory_space=pltpu.SMEM),
            pl.BlockSpec(memory_space=pl.ANY),
        ],
        out_specs=(pl.BlockSpec(memory_space=pl.ANY), pl.BlockSpec(memory_space=pltpu.VMEM)),
        scratch_shapes=[
            pltpu.VMEM((STAGES, rows + PAD, 2, width), bf16),
            pltpu.VMEM((chunks, 2, 3, N_Q, rows, LANES), bf16),
            pltpu.VMEM((chunks, N_Q, 2, tile_rows, LANES), bf16),
            pltpu.VMEM((chunks, N_Q, 2, tile_rows, LANES), bf16),
            pltpu.VMEM((N_Q, count, probes.shape[1]), bf16),
            pltpu.VMEM((chunks, count, 2 * LANES), f32),
            pltpu.VMEM((chunks, half, 2 * LANES), f32),
            pltpu.VMEM((chunks, N_Q, each, LANES), bf16),
            pltpu.VMEM((N_Q, chunks, each, LANES), bf16),
            dma((STAGES,)), dma, dma((chunks,)), dma((chunks,)), dma, dma((chunks,)),
            dma((2 * N_Z,)), dma, dma, dma, dma,
            dma, dma((chunks,)), dma, dma, dma,
        ],
        compiler_params=pltpu.CompilerParams(has_side_effects=True, vmem_limit_bytes=62 * 2**20),
        name="reshard_check",
    )(jnp.transpose(flat_shards, (0, 2, 1, 3)), offsets, probes)


def solution(mesh):
    placed = (P(None, None, ("grp", "tp"), None), P(), P(None, "grp"))
    return jax.shard_map(
        per_device,
        mesh=mesh,
        in_specs=placed,
        out_specs=(P(None, None, "grp", "tp"), P(None, "grp", "tp")),
        check_vma=False,
    )
```

```python
import functools

import jax
import jax.numpy as jnp
from jax import lax
from jax.experimental import pallas as pl
from jax.experimental.pallas import tpu as pltpu
from jax.sharding import PartitionSpec as P

PAD = 2
LANES = 128
N_Y = 4
N_Z = 4
N_Q = N_Y * N_Z
STAGES = 4
LAG = 3
MESH = pl.DeviceIdType.MESH

STEPS = (
    (2, 2), (1, 0), (0, 1), (3, 0), (0, 3), (2, 1), (1, 2), (2, 3),
    (3, 2), (1, 1), (3, 3), (2, 0), (0, 2), (1, 3), (3, 1),
)


def kernel(
    layers, flat, offsets, probes, tile, check,
    stage, to_tp, column, features, total, other, gated,
    stage_sem, send_a, recv_n, recv_a, send_b, recv_b, own_p, send_p, recv_p, send_f, recv_f,
    send_r, recv_r, send_h, recv_h,
):
    tp = lax.axis_index("tp")
    grp = lax.axis_index("grp")
    core = lax.rem(tp, 2)
    z, x_lo, y = grp // 8, lax.rem(grp // 4, 2), lax.rem(grp, 4)
    mine = z * N_Y + y
    rows = to_tp.shape[4]
    blocks = to_tp.shape[3]
    chunks = tile.shape[0]
    per_layer = chunks // layers
    width = blocks * LANES
    tile_cols = per_layer * width
    pair = 2 * rows
    half = other.shape[1]
    each = half // N_Q

    def peer(dz, dy):
        z2, y2 = lax.rem(z + dz, N_Z), lax.rem(y + dy, N_Y)
        return z2 * N_Y + y2, {"grp": z2 * 8 + x_lo * 4 + y2}

    def remote(src, dst, send, recv, where):
        return pltpu.make_async_remote_copy(
            src_ref=src, dst_ref=dst, send_sem=send, recv_sem=recv,
            device_id=where, device_id_type=MESH,
        )

    def drained(ref, sem):
        pltpu.make_async_copy(ref, ref, sem).wait()

    barrier = pltpu.get_barrier_semaphore()
    partner = {"grp": grp + 4 - 8 * x_lo}
    met = [partner] + [{"tp": lax.rem(tp + by, 4)} for by in (1, 2, 3)] + [peer(dz, dy)[1] for dz, dy in STEPS]
    for where in met:
        pl.semaphore_signal(barrier, inc=1, device_id=where, device_id_type=MESH)

    units = chunks * 4

    def unit_of(u):
        chunk, step = u // 4, lax.rem(u, 4)
        far = 2 - 2 * (tp // 2) + lax.rem(core + step, 2)
        near = 2 * (tp // 2) + lax.rem(core + step + 1, 2)
        return chunk, step, jnp.where(step < 2, far, near)

    def fetch(u):
        chunk, step, dest = unit_of(u)
        start = dest * tile_cols + lax.rem(chunk, per_layer) * width
        slot = lax.rem(u, STAGES)
        return pltpu.make_async_copy(
            flat.at[chunk // per_layer, :, :, pl.ds(pl.multiple_of(start, LANES), width)],
            stage.at[slot], stage_sem.at[slot],
        )

    for u in range(STAGES):
        fetch(u).start()

    group = N_Y * each
    own = [
        pltpu.make_async_copy(
            probes.at[pl.ds((at * 2 + lo) * group, group)],
            features.at[z, y, pl.ds(lo * half + at * group, group)],
            own_p.at[at * 2 + lo],
        )
        for at in range(N_Z) for lo in range(2)
    ]
    for copy in own:
        copy.start()
    for copy in own:
        copy.wait()
    pl.semaphore_wait(barrier, len(met))
    share = pl.ds(pl.multiple_of(core * half, half), half)
    along_y = pl.ds(pl.multiple_of(core * half, half // 2), half // 2)
    along_z = pl.ds(pl.multiple_of(core * half + half // 2, half // 2), half // 2)

    def share_own():
        for by in (2, 1, 3):
            _, where_y = peer(0, by)
            _, where_z = peer(by, 0)
            for rows_of, where in ((along_y, where_y), (along_z, where_z)):
                block = features.at[z, y, rows_of]
                remote(block, block, send_p, recv_p.at[0], where).start()

    def share_lines():
        drained(features.at[0, pl.ds(0, 3), share], recv_p.at[0])
        for by in (2, 1, 3):
            _, where_y = peer(0, by)
            _, where_z = peer(by, 0)
            for line, where in ((features.at[z, :, along_y], where_z), (features.at[:, y, along_z], where_y)):
                remote(line, line, send_p, recv_p.at[1], where).start()

    share_own()

    held = stage.shape[1]
    row = lax.broadcasted_iota(jnp.int32, (pair, 2 * held), 0)
    col = lax.broadcasted_iota(jnp.int32, (pair, 2 * held), 1)

    own_rows = pl.ds(pl.multiple_of(tp * rows, rows), rows)
    near_rows = pl.ds(pl.multiple_of((tp // 2) * pair, pair), pair)
    far_rows = pl.ds(pl.multiple_of((1 - tp // 2) * pair, pair), pair)

    def pick(u, _):
        chunk, step, dest = unit_of(u)
        slot = lax.rem(u, STAGES)
        fetch(u).wait()
        layer = chunk // per_layer
        wanted = jnp.where(row < rows, 2 * (row + offsets[layer, 0]), 2 * (row - rows + offsets[layer, 1]) + 1)
        chosen = jnp.where(col == wanted, 1.0, 0.0).astype(jnp.bfloat16)

        def picked(store):
            for at in range(0, blocks, 2):
                both = stage[slot, :, :, at * LANES:(at + 2) * LANES].reshape(2 * held, 2 * LANES)
                out = jnp.dot(chosen, both, preferred_element_type=jnp.float32).astype(jnp.bfloat16)
                for block in range(2):
                    for tensor in range(2):
                        store(at + block, tensor, out[
                            tensor * rows:(tensor + 1) * rows, block * LANES:(block + 1) * LANES
                        ])

        def send(recv):
            def store(block, tensor, value):
                to_tp[chunk, tensor, step, block] = value

            picked(store)
            for tensor in range(2):
                remote(
                    to_tp.at[chunk, tensor, step], tile.at[chunk, :, tensor, own_rows],
                    send_a, recv.at[chunk], {"tp": dest},
                ).start()

        @pl.when(step < 2)
        def _():
            send(recv_a)

        @pl.when(step == 2)
        def _():
            send(recv_n)

        @pl.when(step == 3)
        def _():
            def store(block, tensor, value):
                tile[chunk, block, tensor, own_rows] = value

            picked(store)

        @pl.when(u + STAGES < units)
        def _():
            fetch(u + STAGES).start()

        return 0

    def spread(chunk, which):
        for dz, dy in STEPS:
            at, where = peer(dz, dy)
            remote(
                tile.at[chunk, at, :, which], column.at[chunk, mine, :, which],
                send_b, recv_b.at[chunk], where,
            ).start()

    def spread_near(chunk):
        drained(to_tp.at[0, :, 0], recv_n.at[chunk])
        spread(chunk, near_rows)

    def picks(chunk, _):
        lax.fori_loop(chunk * 4, chunk * 4 + 4, pick, 0)

        @pl.when(chunk > 0)
        def _():
            spread_near(chunk - 1)

        @pl.when(chunk == 2)
        def _():
            share_lines()

        return 0

    lax.fori_loop(0, chunks, picks, 0)
    spread_near(chunks - 1)

    drained(features.at[pl.ds(0, 3), :, share], recv_p.at[1])
    neighbour = {"tp": tp + 1 - 2 * core}

    def hand_on(step, _):
        at = lax.rem(mine + step + 1, N_Q)
        block = features.at[at // N_Y, lax.rem(at, N_Y), share]
        remote(block, block, send_f, recv_f, neighbour).start()
        return 0

    lax.fori_loop(0, N_Q - 1, hand_on, 0)
    others = column.at[0, pl.ds(0, N_Q - 1)]
    drained(others, recv_f)

    def spread_far(chunk):
        drained(to_tp.at[0, :, pl.ds(0, 2)], recv_a.at[chunk])
        spread(chunk, far_rows)
        column[chunk, mine] = tile[chunk, mine]

    keep = pl.ds(pl.multiple_of(x_lo * half, half), half)
    give = pl.ds(pl.multiple_of((1 - x_lo) * half, half), half)

    def multiply(chunk):
        drained(column.at[chunk, pl.ds(0, N_Q - 1)], recv_b.at[chunk])

        def product(part):
            total[chunk, part] = jnp.zeros(other.shape[1:], jnp.float32)

            def add(at, _):
                weights = jnp.concatenate([column[chunk, at, 0], column[chunk, at, 1]], axis=1)
                total[chunk, part] += jnp.dot(
                    features[at // N_Y, lax.rem(at, N_Y), part], weights, preferred_element_type=jnp.float32
                )
                return 0

            lax.fori_loop(0, N_Q, add, 0)

        product(give)
        remote(total.at[chunk, give], other.at[chunk], send_r, recv_r.at[chunk], partner).start()
        product(keep)

    def gate(chunk):
        drained(other.at[chunk], recv_r.at[chunk])
        sums = total[chunk, keep] + other[chunk]
        v, up = sums[:, :LANES], sums[:, LANES:]
        hidden = (v / (1.0 + jnp.exp(-v)) * up).astype(jnp.bfloat16)
        gated[chunk] = hidden.reshape(N_Q, each, LANES)
        check[mine, chunk] = gated[chunk, mine]
        for dz, dy in STEPS:
            at, where = peer(dz, dy)
            remote(gated.at[chunk, at], check.at[mine, chunk], send_h, recv_h, where).start()

    def step(chunk, _):
        spread_far(chunk)

        @pl.when(chunk >= LAG)
        def _():
            multiply(chunk - LAG)

        return 0

    def finish(chunk, _):
        multiply(chunk)
        gate(chunk - LAG)
        return 0

    lax.fori_loop(0, chunks, step, 0)
    lax.fori_loop(chunks - LAG, chunks, finish, 0)
    for chunk in range(chunks - LAG, chunks):
        gate(chunk)

    arrived = check.at[pl.ds(0, N_Q - 1)]
    drained(arrived, recv_h)
    drained(to_tp, send_a)
    drained(column.at[:, pl.ds(0, N_Q - 1)], send_b)
    for sem in (send_p, send_f):
        drained(others, sem)
    drained(other, send_r)
    drained(arrived, send_h)


def place(tile, check, tiles_out, check_out, sem):
    chunks, blocks = tile.shape[:2]
    layers = tiles_out.shape[0]
    per_layer = chunks // layers
    copies = []
    for chunk in range(chunks):
        for block in range(blocks):
            start = (chunk % per_layer * blocks + block) * LANES
            for tensor in range(2):
                copy = pltpu.make_async_copy(
                    tile.at[chunk, block, tensor],
                    tiles_out.at[chunk // per_layer, tensor, :, pl.ds(start, LANES)],
                    sem,
                )
                copy.start()
            check_out[chunk // per_layer, :, start:start + LANES] = check[block, chunk]
    pltpu.make_async_copy(tile, tile, sem).wait()


def per_device(flat_shards, offsets, probes):
    tp_count = lax.axis_size("tp")
    layers = flat_shards.shape[0]
    rows = flat_shards.shape[2] - PAD
    tile_cols = flat_shards.shape[3] // tp_count
    tile_rows = rows * tp_count
    count = probes.shape[0]
    half = count // 2
    each = half // N_Q
    width = N_Q * LANES
    chunks = layers * (tile_cols // width)
    bf16, f32 = jnp.bfloat16, jnp.float32
    dma = pltpu.SemaphoreType.DMA
    tile, check = pl.pallas_call(
        functools.partial(kernel, layers),
        out_shape=(
            pltpu.VMEM((chunks, N_Q, 2, tile_rows, LANES), bf16),
            pltpu.VMEM((N_Q, chunks, each, LANES), bf16),
        ),
        in_specs=[
            pl.BlockSpec(memory_space=pl.ANY),
            pl.BlockSpec(memory_space=pltpu.SMEM),
            pl.BlockSpec(memory_space=pl.ANY),
        ],
        out_specs=(pl.BlockSpec(memory_space=pltpu.VMEM), pl.BlockSpec(memory_space=pltpu.VMEM)),
        scratch_shapes=[
            pltpu.VMEM((STAGES, rows + PAD, 2, width), bf16),
            pltpu.VMEM((chunks, 2, 3, N_Q, rows, LANES), bf16),
            pltpu.VMEM((chunks, N_Q, 2, tile_rows, LANES), bf16),
            pltpu.VMEM((N_Z, N_Y, count, probes.shape[1]), bf16),
            pltpu.VMEM((chunks, count, 2 * LANES), f32),
            pltpu.VMEM((chunks, half, 2 * LANES), f32),
            pltpu.VMEM((chunks, N_Q, each, LANES), bf16),
            dma((STAGES,)), dma, dma((chunks,)), dma((chunks,)), dma, dma((chunks,)),
            dma((2 * N_Z,)), dma, dma((2,)), dma, dma,
            dma, dma((chunks,)), dma, dma,
        ],
        compiler_params=pltpu.CompilerParams(
            collective_id=0, has_side_effects=True, vmem_limit_bytes=51 * 2**20
        ),
        name="reshard_check",
    )(jnp.transpose(flat_shards, (0, 2, 1, 3)), offsets, probes)
    return pl.pallas_call(
        place,
        out_shape=(
            jax.ShapeDtypeStruct((layers, 2, tile_rows, tile_cols), bf16),
            jax.ShapeDtypeStruct((layers, each, tile_cols), bf16),
        ),
        in_specs=[pl.BlockSpec(memory_space=pltpu.VMEM), pl.BlockSpec(memory_space=pltpu.VMEM)],
        out_specs=(pl.BlockSpec(memory_space=pl.ANY), pl.BlockSpec(memory_space=pltpu.VMEM)),
        scratch_shapes=[dma],
        compiler_params=pltpu.CompilerParams(vmem_limit_bytes=16 * 2**20),
        name="place",
    )(tile, check)


def solution(mesh):
    placed = (P(None, None, ("grp", "tp"), None), P(), P(None, "grp"))
    return jax.shard_map(
        per_device,
        mesh=mesh,
        in_specs=placed,
        out_specs=(P(None, None, "grp", "tp"), P(None, "grp", "tp")),
        check_vma=False,
    )
```

```python
import functools

import jax
import jax.numpy as jnp
from jax import lax
from jax.experimental import pallas as pl
from jax.experimental.pallas import tpu as pltpu
from jax.sharding import PartitionSpec as P

PAD = 2
LANES = 128
N_Y = 4
N_Z = 4
N_Q = N_Y * N_Z
STAGES = 4
LAG = 3
MESH = pl.DeviceIdType.MESH

STEPS = (
    (2, 2), (1, 0), (0, 1), (3, 0), (0, 3), (2, 1), (1, 2), (2, 3),
    (3, 2), (1, 1), (3, 3), (2, 0), (0, 2), (1, 3), (3, 1),
)


def kernel(
    layers, flat, offsets, probes, tile, check,
    stage, to_tp, column, features, total, other, gated,
    stage_sem, send_a, recv_n, recv_a, send_b, recv_b, own_p, send_p, recv_p, send_f, recv_f,
    send_r, recv_r, send_h, recv_h,
):
    tp = lax.axis_index("tp")
    grp = lax.axis_index("grp")
    core = lax.rem(tp, 2)
    z, x_lo, y = grp // 8, lax.rem(grp // 4, 2), lax.rem(grp, 4)
    mine = z * N_Y + y
    rows = to_tp.shape[4]
    blocks = to_tp.shape[3]
    chunks = tile.shape[0]
    per_layer = chunks // layers
    width = blocks * LANES
    tile_cols = per_layer * width
    pair = 2 * rows
    half = other.shape[1]
    each = half // N_Q

    def peer(dz, dy):
        z2, y2 = lax.rem(z + dz, N_Z), lax.rem(y + dy, N_Y)
        return z2 * N_Y + y2, {"grp": z2 * 8 + x_lo * 4 + y2}

    def remote(src, dst, send, recv, where):
        return pltpu.make_async_remote_copy(
            src_ref=src, dst_ref=dst, send_sem=send, recv_sem=recv,
            device_id=where, device_id_type=MESH,
        )

    def drained(ref, sem):
        pltpu.make_async_copy(ref, ref, sem).wait()

    barrier = pltpu.get_barrier_semaphore()
    partner = {"grp": grp + 4 - 8 * x_lo}
    met = [partner] + [{"tp": lax.rem(tp + by, 4)} for by in (1, 2, 3)] + [peer(dz, dy)[1] for dz, dy in STEPS]
    for where in met:
        pl.semaphore_signal(barrier, inc=1, device_id=where, device_id_type=MESH)

    units = chunks * 4

    def unit_of(u):
        chunk, step = u // 4, lax.rem(u, 4)
        far = 2 - 2 * (tp // 2) + lax.rem(core + step, 2)
        near = 2 * (tp // 2) + lax.rem(core + step + 1, 2)
        return chunk, step, jnp.where(step < 2, far, near)

    def fetch(u):
        chunk, step, dest = unit_of(u)
        start = dest * tile_cols + lax.rem(chunk, per_layer) * width
        slot = lax.rem(u, STAGES)
        return pltpu.make_async_copy(
            flat.at[chunk // per_layer, :, :, pl.ds(pl.multiple_of(start, LANES), width)],
            stage.at[slot], stage_sem.at[slot],
        )

    for u in range(STAGES):
        fetch(u).start()

    group = N_Y * each
    own = [
        pltpu.make_async_copy(
            probes.at[pl.ds((at * 2 + lo) * group, group)],
            features.at[z, y, pl.ds(lo * half + at * group, group)],
            own_p.at[at * 2 + lo],
        )
        for at in range(N_Z) for lo in range(2)
    ]
    for copy in own:
        copy.start()
    share = pl.ds(pl.multiple_of(core * half, half), half)
    along_y = pl.ds(pl.multiple_of(core * half, half // 2), half // 2)
    along_z = pl.ds(pl.multiple_of(core * half + half // 2, half // 2), half // 2)

    def share_own():
        for by in (2, 1, 3):
            _, where_y = peer(0, by)
            _, where_z = peer(by, 0)
            for rows_of, where in ((along_y, where_y), (along_z, where_z)):
                block = features.at[z, y, rows_of]
                remote(block, block, send_p, recv_p.at[0], where).start()

    def share_lines():
        drained(features.at[0, pl.ds(0, 3), share], recv_p.at[0])
        for by in (2, 1, 3):
            _, where_y = peer(0, by)
            _, where_z = peer(by, 0)
            for line, where in ((features.at[z, :, along_y], where_z), (features.at[:, y, along_z], where_y)):
                remote(line, line, send_p, recv_p.at[1], where).start()

    held = stage.shape[1]
    row = lax.broadcasted_iota(jnp.int32, (pair, 2 * held), 0)
    col = lax.broadcasted_iota(jnp.int32, (pair, 2 * held), 1)

    own_rows = pl.ds(pl.multiple_of(tp * rows, rows), rows)
    near_rows = pl.ds(pl.multiple_of((tp // 2) * pair, pair), pair)
    far_rows = pl.ds(pl.multiple_of((1 - tp // 2) * pair, pair), pair)

    def pick(u):
        chunk, step, dest = unit_of(u)
        slot = lax.rem(u, STAGES)
        fetch(u).wait()
        layer = chunk // per_layer
        wanted = jnp.where(row < rows, 2 * (row + offsets[layer, 0]), 2 * (row - rows + offsets[layer, 1]) + 1)
        chosen = jnp.where(col == wanted, 1.0, 0.0).astype(jnp.bfloat16)

        def picked(store):
            for at in range(0, blocks, 2):
                both = stage[slot, :, :, at * LANES:(at + 2) * LANES].reshape(2 * held, 2 * LANES)
                out = jnp.dot(chosen, both, preferred_element_type=jnp.float32).astype(jnp.bfloat16)
                for block in range(2):
                    for tensor in range(2):
                        store(at + block, tensor, out[
                            tensor * rows:(tensor + 1) * rows, block * LANES:(block + 1) * LANES
                        ])

        @pl.when(step < 3)
        def _():
            def store(block, tensor, value):
                to_tp[chunk, tensor, step, block] = value

            picked(store)

        @pl.when(step == 3)
        def _():
            def store(block, tensor, value):
                tile[chunk, block, tensor, own_rows] = value

            picked(store)

        @pl.when(u + STAGES < units)
        def _():
            fetch(u + STAGES).start()

    def ship(u, _):
        chunk, step, dest = unit_of(u)

        def send(recv):
            for tensor in range(2):
                remote(
                    to_tp.at[chunk, tensor, step], tile.at[chunk, :, tensor, own_rows],
                    send_a, recv.at[chunk], {"tp": dest},
                ).start()

        @pl.when(step < 2)
        def _():
            send(recv_a)

        @pl.when(step == 2)
        def _():
            send(recv_n)

        @pl.when(u + 1 < units)
        def _():
            pick(u + 1)

        return 0

    def spread(chunk, which):
        for dz, dy in STEPS:
            at, where = peer(dz, dy)
            remote(
                tile.at[chunk, at, :, which], column.at[chunk, mine, :, which],
                send_b, recv_b.at[chunk], where,
            ).start()

    def spread_near(chunk):
        drained(to_tp.at[0, :, 0], recv_n.at[chunk])
        spread(chunk, near_rows)

    def picks(chunk, _):
        lax.fori_loop(chunk * 4, chunk * 4 + 4, ship, 0)

        @pl.when(chunk > 0)
        def _():
            spread_near(chunk - 1)

        @pl.when(chunk == 2)
        def _():
            share_lines()

        return 0

    pick(0)
    for copy in own:
        copy.wait()
    pl.semaphore_wait(barrier, len(met))
    share_own()
    lax.fori_loop(0, chunks, picks, 0)
    spread_near(chunks - 1)

    drained(features.at[pl.ds(0, 3), :, share], recv_p.at[1])
    neighbour = {"tp": tp + 1 - 2 * core}

    def hand_on(step, _):
        at = lax.rem(mine + step + 1, N_Q)
        block = features.at[at // N_Y, lax.rem(at, N_Y), share]
        remote(block, block, send_f, recv_f, neighbour).start()
        return 0

    lax.fori_loop(0, N_Q - 1, hand_on, 0)
    others = column.at[0, pl.ds(0, N_Q - 1)]
    drained(others, recv_f)

    def spread_far(chunk):
        drained(to_tp.at[0, :, pl.ds(0, 2)], recv_a.at[chunk])
        spread(chunk, far_rows)
        column[chunk, mine] = tile[chunk, mine]

    keep = pl.ds(pl.multiple_of(x_lo * half, half), half)
    give = pl.ds(pl.multiple_of((1 - x_lo) * half, half), half)

    def multiply(chunk):
        drained(column.at[chunk, pl.ds(0, N_Q - 1)], recv_b.at[chunk])

        def product(turn, _):
            part = pl.ds(pl.multiple_of(lax.rem(1 - x_lo + turn, 2) * half, half), half)
            left = jnp.concatenate([features[at // N_Y, at % N_Y, part] for at in range(N_Q)], axis=1)
            right = jnp.concatenate([
                jnp.concatenate([column[chunk, at, 0], column[chunk, at, 1]], axis=1) for at in range(N_Q)
            ], axis=0)
            total[chunk, part] = jnp.dot(left, right, preferred_element_type=jnp.float32)

            @pl.when(turn == 0)
            def _():
                remote(total.at[chunk, give], other.at[chunk], send_r, recv_r.at[chunk], partner).start()

            return 0

        lax.fori_loop(0, 2, product, 0)

    def gate(chunk):
        drained(other.at[chunk], recv_r.at[chunk])
        sums = total[chunk, keep] + other[chunk]
        v, up = sums[:, :LANES], sums[:, LANES:]
        hidden = (v / (1.0 + jnp.exp(-v)) * up).astype(jnp.bfloat16)
        gated[chunk] = hidden.reshape(N_Q, each, LANES)
        check[mine, chunk] = gated[chunk, mine]
        for dz, dy in STEPS:
            at, where = peer(dz, dy)
            remote(gated.at[chunk, at], check.at[mine, chunk], send_h, recv_h, where).start()

    def step(chunk, _):
        spread_far(chunk)

        @pl.when(chunk >= LAG)
        def _():
            multiply(chunk - LAG)

        return 0

    def finish(chunk, _):
        multiply(chunk)
        gate(chunk - LAG)
        return 0

    lax.fori_loop(0, chunks, step, 0)
    lax.fori_loop(chunks - LAG, chunks, finish, 0)
    for chunk in range(chunks - LAG, chunks):
        gate(chunk)

    arrived = check.at[pl.ds(0, N_Q - 1)]
    drained(arrived, recv_h)
    drained(to_tp, send_a)
    drained(column.at[:, pl.ds(0, N_Q - 1)], send_b)
    for sem in (send_p, send_f):
        drained(others, sem)
    drained(other, send_r)
    drained(arrived, send_h)


def place(tile, check, tiles_out, check_out, lines, sem, line_sem):
    chunks, blocks = tile.shape[:2]
    layers = tiles_out.shape[0]
    per_layer = chunks // layers
    for chunk in range(chunks):
        for block in range(blocks):
            start = (chunk % per_layer * blocks + block) * LANES
            for tensor in range(2):
                copy = pltpu.make_async_copy(
                    tile.at[chunk, block, tensor],
                    tiles_out.at[chunk // per_layer, tensor, :, pl.ds(start, LANES)],
                    sem,
                )
                copy.start()
            lines[chunk // per_layer, :, start:start + LANES] = check[block, chunk]
    copy = pltpu.make_async_copy(lines, check_out, line_sem)
    copy.start()
    copy.wait()
    pltpu.make_async_copy(tile, tile, sem).wait()


def per_device(flat_shards, offsets, probes):
    tp_count = lax.axis_size("tp")
    layers = flat_shards.shape[0]
    rows = flat_shards.shape[2] - PAD
    tile_cols = flat_shards.shape[3] // tp_count
    tile_rows = rows * tp_count
    count = probes.shape[0]
    half = count // 2
    each = half // N_Q
    width = N_Q * LANES
    chunks = layers * (tile_cols // width)
    bf16, f32 = jnp.bfloat16, jnp.float32
    dma = pltpu.SemaphoreType.DMA
    tile, check = pl.pallas_call(
        functools.partial(kernel, layers),
        out_shape=(
            pltpu.VMEM((chunks, N_Q, 2, tile_rows, LANES), bf16),
            pltpu.VMEM((N_Q, chunks, each, LANES), bf16),
        ),
        in_specs=[
            pl.BlockSpec(memory_space=pl.ANY),
            pl.BlockSpec(memory_space=pltpu.SMEM),
            pl.BlockSpec(memory_space=pl.ANY),
        ],
        out_specs=(pl.BlockSpec(memory_space=pltpu.VMEM), pl.BlockSpec(memory_space=pltpu.VMEM)),
        scratch_shapes=[
            pltpu.VMEM((STAGES, rows + PAD, 2, width), bf16),
            pltpu.VMEM((chunks, 2, 3, N_Q, rows, LANES), bf16),
            pltpu.VMEM((chunks, N_Q, 2, tile_rows, LANES), bf16),
            pltpu.VMEM((N_Z, N_Y, count, probes.shape[1]), bf16),
            pltpu.VMEM((chunks, count, 2 * LANES), f32),
            pltpu.VMEM((chunks, half, 2 * LANES), f32),
            pltpu.VMEM((chunks, N_Q, each, LANES), bf16),
            dma((STAGES,)), dma, dma((chunks,)), dma((chunks,)), dma, dma((chunks,)),
            dma((2 * N_Z,)), dma, dma((2,)), dma, dma,
            dma, dma((chunks,)), dma, dma,
        ],
        compiler_params=pltpu.CompilerParams(
            collective_id=0, has_side_effects=True, vmem_limit_bytes=51 * 2**20
        ),
        name="reshard_check",
    )(jnp.transpose(flat_shards, (0, 2, 1, 3)), offsets, probes)
    return pl.pallas_call(
        place,
        out_shape=(
            jax.ShapeDtypeStruct((layers, 2, tile_rows, tile_cols), bf16),
            jax.ShapeDtypeStruct((layers, each, tile_cols), bf16),
        ),
        in_specs=[pl.BlockSpec(memory_space=pltpu.VMEM), pl.BlockSpec(memory_space=pltpu.VMEM)],
        out_specs=(pl.BlockSpec(memory_space=pl.ANY), pl.BlockSpec(memory_space=pl.ANY)),
        scratch_shapes=[pltpu.VMEM((layers, each, tile_cols), bf16), dma, dma],
        compiler_params=pltpu.CompilerParams(vmem_limit_bytes=16 * 2**20),
        name="place",
    )(tile, check)


def solution(mesh):
    placed = (P(None, None, ("grp", "tp"), None), P(), P(None, "grp"))
    return jax.shard_map(
        per_device,
        mesh=mesh,
        in_specs=placed,
        out_specs=(P(None, None, "grp", "tp"), P(None, "grp", "tp")),
        check_vma=False,
    )
```

```python
import functools

import jax
import jax.numpy as jnp
from jax import lax
from jax.experimental import pallas as pl
from jax.experimental.pallas import tpu as pltpu
from jax.sharding import PartitionSpec as P

PAD = 2
LANES = 128
N_Y = 4
N_Z = 4
N_Q = N_Y * N_Z
STAGES = 4
LAG = 3
MESH = pl.DeviceIdType.MESH

STEPS = (
    (2, 2), (1, 0), (0, 1), (3, 0), (0, 3), (2, 1), (1, 2), (2, 3),
    (3, 2), (1, 1), (3, 3), (2, 0), (0, 2), (1, 3), (3, 1),
)


def kernel(
    layers, flat, offsets, probes, tile, check,
    stage, to_tp, column, features, total, other, gated, ends,
    stage_sem, send_a, recv_n, recv_a, send_b, recv_b, own_p, send_p, recv_p, send_f, recv_f,
    send_r, recv_r, send_h, recv_h, send_e, recv_e,
):
    tp = lax.axis_index("tp")
    grp = lax.axis_index("grp")
    core = lax.rem(tp, 2)
    z, x_lo, y = grp // 8, lax.rem(grp // 4, 2), lax.rem(grp, 4)
    mine = z * N_Y + y
    rows = to_tp.shape[4]
    blocks = to_tp.shape[3]
    chunks = tile.shape[0]
    per_layer = chunks // layers
    width = blocks * LANES
    tile_cols = per_layer * width
    pair = 2 * rows
    half = other.shape[1]
    each = half // N_Q

    def peer(dz, dy):
        z2, y2 = lax.rem(z + dz, N_Z), lax.rem(y + dy, N_Y)
        return z2 * N_Y + y2, {"grp": z2 * 8 + x_lo * 4 + y2}

    def remote(src, dst, send, recv, where):
        return pltpu.make_async_remote_copy(
            src_ref=src, dst_ref=dst, send_sem=send, recv_sem=recv,
            device_id=where, device_id_type=MESH,
        )

    def drained(ref, sem):
        pltpu.make_async_copy(ref, ref, sem).wait()

    barrier = pltpu.get_barrier_semaphore()
    partner = {"grp": grp + 4 - 8 * x_lo}
    met = [partner] + [{"tp": lax.rem(tp + by, 4)} for by in (1, 2, 3)]
    for dz, dy in STEPS:
        where = peer(dz, dy)[1]["grp"]
        met += [{"grp": where}, {"grp": where + 4 - 8 * x_lo}]
    for where in met:
        pl.semaphore_signal(barrier, inc=1, device_id=where, device_id_type=MESH)

    units = chunks * 4

    def unit_of(u):
        chunk, step = u // 4, lax.rem(u, 4)
        far = 2 - 2 * (tp // 2) + lax.rem(core + step, 2)
        near = 2 * (tp // 2) + lax.rem(core + step + 1, 2)
        return chunk, step, jnp.where(step < 2, far, near)

    def fetch(u):
        chunk, step, dest = unit_of(u)
        start = dest * tile_cols + lax.rem(chunk, per_layer) * width
        slot = lax.rem(u, STAGES)
        return pltpu.make_async_copy(
            flat.at[chunk // per_layer, :, :, pl.ds(pl.multiple_of(start, LANES), width)],
            stage.at[slot], stage_sem.at[slot],
        )

    for u in range(STAGES):
        fetch(u).start()

    group = N_Y * each
    own = [
        pltpu.make_async_copy(
            probes.at[pl.ds((at * 2 + lo) * group, group)],
            features.at[z, y, pl.ds(lo * half + at * group, group)],
            own_p.at[at * 2 + lo],
        )
        for at in range(N_Z) for lo in range(2)
    ]
    for copy in own:
        copy.start()
    share = pl.ds(pl.multiple_of(core * half, half), half)
    along_y = pl.ds(pl.multiple_of(core * half, half // 2), half // 2)
    along_z = pl.ds(pl.multiple_of(core * half + half // 2, half // 2), half // 2)

    def share_own():
        for by in (2, 1, 3):
            _, where_y = peer(0, by)
            _, where_z = peer(by, 0)
            for rows_of, where in ((along_y, where_y), (along_z, where_z)):
                block = features.at[z, y, rows_of]
                remote(block, block, send_p, recv_p.at[0], where).start()

    def share_lines():
        drained(features.at[0, pl.ds(0, 3), share], recv_p.at[0])
        for by in (2, 1, 3):
            _, where_y = peer(0, by)
            _, where_z = peer(by, 0)
            for line, where in ((features.at[z, :, along_y], where_z), (features.at[:, y, along_z], where_y)):
                remote(line, line, send_p, recv_p.at[1], where).start()

    held = stage.shape[1]
    row = lax.broadcasted_iota(jnp.int32, (pair, 2 * held), 0)
    col = lax.broadcasted_iota(jnp.int32, (pair, 2 * held), 1)

    own_rows = pl.ds(pl.multiple_of(tp * rows, rows), rows)
    near_rows = pl.ds(pl.multiple_of((tp // 2) * pair, pair), pair)
    far_rows = pl.ds(pl.multiple_of((1 - tp // 2) * pair, pair), pair)

    def pick(u):
        chunk, step, dest = unit_of(u)
        slot = lax.rem(u, STAGES)
        fetch(u).wait()
        layer = chunk // per_layer
        wanted = jnp.where(row < rows, 2 * (row + offsets[layer, 0]), 2 * (row - rows + offsets[layer, 1]) + 1)
        chosen = jnp.where(col == wanted, 1.0, 0.0).astype(jnp.bfloat16)

        def picked(store):
            for at in range(0, blocks, 2):
                both = stage[slot, :, :, at * LANES:(at + 2) * LANES].reshape(2 * held, 2 * LANES)
                out = jnp.dot(chosen, both, preferred_element_type=jnp.float32).astype(jnp.bfloat16)
                for block in range(2):
                    for tensor in range(2):
                        store(at + block, tensor, out[
                            tensor * rows:(tensor + 1) * rows, block * LANES:(block + 1) * LANES
                        ])

        @pl.when(step < 3)
        def _():
            def store(block, tensor, value):
                to_tp[chunk, tensor, step, block] = value

            picked(store)

        @pl.when(step == 3)
        def _():
            def store(block, tensor, value):
                tile[chunk, block, tensor, own_rows] = value

            picked(store)

        @pl.when(u + STAGES < units)
        def _():
            fetch(u + STAGES).start()

    def ship(u, _):
        chunk, step, dest = unit_of(u)

        def send(recv):
            for tensor in range(2):
                remote(
                    to_tp.at[chunk, tensor, step], tile.at[chunk, :, tensor, own_rows],
                    send_a, recv.at[chunk], {"tp": dest},
                ).start()

        @pl.when(step < 2)
        def _():
            send(recv_a)

        @pl.when(step == 2)
        def _():
            send(recv_n)

        @pl.when(u + 1 < units)
        def _():
            pick(u + 1)

        return 0

    def spread(chunk, which):
        for dz, dy in STEPS:
            at, where = peer(dz, dy)
            remote(
                tile.at[chunk, at, :, which], column.at[chunk, mine, :, which],
                send_b, recv_b.at[chunk], where,
            ).start()

    def spread_near(chunk):
        drained(to_tp.at[0, :, 0], recv_n.at[chunk])
        spread(chunk, near_rows)

    def picks(chunk, _):
        lax.fori_loop(chunk * 4, chunk * 4 + 4, ship, 0)

        @pl.when(chunk > 0)
        def _():
            spread_near(chunk - 1)

        @pl.when(chunk == 2)
        def _():
            share_lines()

        return 0

    pick(0)
    for copy in own:
        copy.wait()
    pl.semaphore_wait(barrier, len(met))
    share_own()
    lax.fori_loop(0, chunks, picks, 0)
    spread_near(chunks - 1)

    drained(features.at[pl.ds(0, 3), :, share], recv_p.at[1])
    neighbour = {"tp": tp + 1 - 2 * core}

    def hand_on(step, _):
        at = lax.rem(mine + step + 1, N_Q)
        block = features.at[at // N_Y, lax.rem(at, N_Y), share]
        remote(block, block, send_f, recv_f, neighbour).start()
        return 0

    lax.fori_loop(0, N_Q - 1, hand_on, 0)
    others = column.at[0, pl.ds(0, N_Q - 1)]
    drained(others, recv_f)

    def spread_far(chunk):
        drained(to_tp.at[0, :, pl.ds(0, 2)], recv_a.at[chunk])
        spread(chunk, far_rows)
        column[chunk, mine] = tile[chunk, mine]

    keep = pl.ds(pl.multiple_of(x_lo * half, half), half)
    give = pl.ds(pl.multiple_of((1 - x_lo) * half, half), half)

    def multiply(chunk):
        drained(column.at[chunk, pl.ds(0, N_Q - 1)], recv_b.at[chunk])

        def product(turn, _):
            part = pl.ds(pl.multiple_of(lax.rem(1 - x_lo + turn, 2) * half, half), half)
            left = jnp.concatenate([features[at // N_Y, at % N_Y, part] for at in range(N_Q)], axis=1)
            right = jnp.concatenate([
                jnp.concatenate([column[chunk, at, 0], column[chunk, at, 1]], axis=1) for at in range(N_Q)
            ], axis=0)
            total[chunk, part] = jnp.dot(left, right, preferred_element_type=jnp.float32)

            @pl.when((turn == 0) & (chunk < chunks - 1))
            def _():
                remote(total.at[chunk, give], other.at[chunk], send_r, recv_r.at[chunk], partner).start()

            @pl.when((turn == 0) & (chunk == chunks - 1))
            def _():
                for dz, dy in STEPS + ((0, 0),):
                    at, where = peer(dz, dy)
                    remote(
                        total.at[chunk, rows_for(1 - x_lo, at)], ends.at[x_lo * N_Q + mine],
                        send_e, recv_e, {"grp": where["grp"] + 4 - 8 * x_lo},
                    ).start()

            @pl.when((turn == 1) & (chunk == chunks - 1))
            def _():
                for dz, dy in STEPS:
                    at, where = peer(dz, dy)
                    remote(
                        total.at[chunk, rows_for(x_lo, at)], ends.at[x_lo * N_Q + mine], send_e, recv_e, where,
                    ).start()

            return 0

        lax.fori_loop(0, 2, product, 0)

    def rows_for(lo, at):
        return pl.ds(pl.multiple_of(lo * half + at * each, each), each)

    def gate_of(sums):
        v, up = sums[..., :LANES], sums[..., LANES:]
        return (v / (1.0 + jnp.exp(-v)) * up).astype(jnp.bfloat16)

    def gate(chunk):
        drained(other.at[chunk], recv_r.at[chunk])
        gated[chunk] = gate_of(total[chunk, keep] + other[chunk]).reshape(N_Q, each, LANES)
        check[mine, chunk] = gated[chunk, mine]
        for dz, dy in STEPS:
            at, where = peer(dz, dy)
            remote(gated.at[chunk, at], check.at[mine, chunk], send_h, recv_h, where).start()

    def step(chunk, _):
        spread_far(chunk)

        @pl.when(chunk >= LAG)
        def _():
            multiply(chunk - LAG)

        return 0

    def finish(chunk, _):
        multiply(chunk)
        gate(chunk - LAG)
        return 0

    lax.fori_loop(0, chunks, step, 0)
    lax.fori_loop(chunks - LAG, chunks, finish, 0)
    for chunk in range(chunks - LAG, chunks - 1):
        gate(chunk)
    ends[x_lo * N_Q + mine] = total[chunks - 1, rows_for(x_lo, mine)]
    came = ends.at[pl.ds(0, 2 * N_Q - 1)]
    drained(came, recv_e)
    last = gate_of(ends[:N_Q] + ends[N_Q:])
    for at in range(N_Q):
        check[at, chunks - 1] = last[at]

    arrived = check.at[pl.ds(0, N_Q - 1), pl.ds(0, chunks - 1)]
    drained(arrived, recv_h)
    drained(to_tp, send_a)
    drained(column.at[:, pl.ds(0, N_Q - 1)], send_b)
    for sem in (send_p, send_f):
        drained(others, sem)
    drained(other.at[pl.ds(0, chunks - 1)], send_r)
    drained(came, send_e)
    drained(arrived, send_h)


def place(tile, check, tiles_out, check_out, lines, sem, line_sem):
    chunks, blocks = tile.shape[:2]
    layers = tiles_out.shape[0]
    per_layer = chunks // layers
    for chunk in range(chunks):
        for block in range(blocks):
            start = (chunk % per_layer * blocks + block) * LANES
            for tensor in range(2):
                copy = pltpu.make_async_copy(
                    tile.at[chunk, block, tensor],
                    tiles_out.at[chunk // per_layer, tensor, :, pl.ds(start, LANES)],
                    sem,
                )
                copy.start()
            lines[chunk // per_layer, :, start:start + LANES] = check[block, chunk]
    copy = pltpu.make_async_copy(lines, check_out, line_sem)
    copy.start()
    copy.wait()
    pltpu.make_async_copy(tile, tile, sem).wait()


def per_device(flat_shards, offsets, probes):
    tp_count = lax.axis_size("tp")
    layers = flat_shards.shape[0]
    rows = flat_shards.shape[2] - PAD
    tile_cols = flat_shards.shape[3] // tp_count
    tile_rows = rows * tp_count
    count = probes.shape[0]
    half = count // 2
    each = half // N_Q
    width = N_Q * LANES
    chunks = layers * (tile_cols // width)
    bf16, f32 = jnp.bfloat16, jnp.float32
    dma = pltpu.SemaphoreType.DMA
    tile, check = pl.pallas_call(
        functools.partial(kernel, layers),
        out_shape=(
            pltpu.VMEM((chunks, N_Q, 2, tile_rows, LANES), bf16),
            pltpu.VMEM((N_Q, chunks, each, LANES), bf16),
        ),
        in_specs=[
            pl.BlockSpec(memory_space=pl.ANY),
            pl.BlockSpec(memory_space=pltpu.SMEM),
            pl.BlockSpec(memory_space=pl.ANY),
        ],
        out_specs=(pl.BlockSpec(memory_space=pltpu.VMEM), pl.BlockSpec(memory_space=pltpu.VMEM)),
        scratch_shapes=[
            pltpu.VMEM((STAGES, rows + PAD, 2, width), bf16),
            pltpu.VMEM((chunks, 2, 3, N_Q, rows, LANES), bf16),
            pltpu.VMEM((chunks, N_Q, 2, tile_rows, LANES), bf16),
            pltpu.VMEM((N_Z, N_Y, count, probes.shape[1]), bf16),
            pltpu.VMEM((chunks, count, 2 * LANES), f32),
            pltpu.VMEM((chunks, half, 2 * LANES), f32),
            pltpu.VMEM((chunks, N_Q, each, LANES), bf16),
            pltpu.VMEM((2 * N_Q, each, 2 * LANES), f32),
            dma((STAGES,)), dma, dma((chunks,)), dma((chunks,)), dma, dma((chunks,)),
            dma((2 * N_Z,)), dma, dma((2,)), dma, dma,
            dma, dma((chunks,)), dma, dma, dma, dma,
        ],
        compiler_params=pltpu.CompilerParams(
            collective_id=0, has_side_effects=True, vmem_limit_bytes=51 * 2**20
        ),
        name="reshard_check",
    )(jnp.transpose(flat_shards, (0, 2, 1, 3)), offsets, probes)
    return pl.pallas_call(
        place,
        out_shape=(
            jax.ShapeDtypeStruct((layers, 2, tile_rows, tile_cols), bf16),
            jax.ShapeDtypeStruct((layers, each, tile_cols), bf16),
        ),
        in_specs=[pl.BlockSpec(memory_space=pltpu.VMEM), pl.BlockSpec(memory_space=pltpu.VMEM)],
        out_specs=(pl.BlockSpec(memory_space=pl.ANY), pl.BlockSpec(memory_space=pl.ANY)),
        scratch_shapes=[pltpu.VMEM((layers, each, tile_cols), bf16), dma, dma],
        compiler_params=pltpu.CompilerParams(vmem_limit_bytes=16 * 2**20),
        name="place",
    )(tile, check)


def solution(mesh):
    placed = (P(None, None, ("grp", "tp"), None), P(), P(None, "grp"))
    return jax.shard_map(
        per_device,
        mesh=mesh,
        in_specs=placed,
        out_specs=(P(None, None, "grp", "tp"), P(None, "grp", "tp")),
        check_vma=False,
    )
```

```python
import functools

import jax
import jax.numpy as jnp
from jax import lax
from jax.experimental import pallas as pl
from jax.experimental.pallas import tpu as pltpu
from jax.sharding import PartitionSpec as P

PAD = 2
LANES = 128
N_Y = 4
N_Z = 4
N_Q = N_Y * N_Z
STAGES = 4
LAG = 3
MESH = pl.DeviceIdType.MESH

STEPS = (
    (2, 2), (1, 0), (0, 1), (3, 0), (0, 3), (2, 1), (1, 2), (2, 3),
    (3, 2), (1, 1), (3, 3), (2, 0), (0, 2), (1, 3), (3, 1),
)


def kernel(
    layers, flat, offsets, probes, tile, check,
    stage, to_tp, column, features, total, other, gated, ends,
    stage_sem, send_a, recv_n, recv_a, send_b, recv_b, own_p, send_p, recv_p, send_f, recv_f,
    send_r, recv_r, send_h, recv_h, send_e, recv_e,
):
    tp = lax.axis_index("tp")
    grp = lax.axis_index("grp")
    core = lax.rem(tp, 2)
    z, x_lo, y = grp // 8, lax.rem(grp // 4, 2), lax.rem(grp, 4)
    mine = z * N_Y + y
    rows = to_tp.shape[4]
    blocks = to_tp.shape[3]
    chunks = tile.shape[0]
    per_layer = chunks // layers
    width = blocks * LANES
    tile_cols = per_layer * width
    pair = 2 * rows
    half = other.shape[1]
    each = half // N_Q

    def peer(dz, dy):
        z2, y2 = lax.rem(z + dz, N_Z), lax.rem(y + dy, N_Y)
        return z2 * N_Y + y2, {"grp": z2 * 8 + x_lo * 4 + y2}

    def remote(src, dst, send, recv, where):
        return pltpu.make_async_remote_copy(
            src_ref=src, dst_ref=dst, send_sem=send, recv_sem=recv,
            device_id=where, device_id_type=MESH,
        )

    def drained(ref, sem):
        pltpu.make_async_copy(ref, ref, sem).wait()

    barrier = pltpu.get_barrier_semaphore()
    partner = {"grp": grp + 4 - 8 * x_lo}
    met = [partner] + [{"tp": lax.rem(tp + by, 4)} for by in (1, 2, 3)]
    for dz, dy in STEPS:
        where = peer(dz, dy)[1]["grp"]
        met += [{"grp": where}, {"grp": where + 4 - 8 * x_lo}]
    for where in met:
        pl.semaphore_signal(barrier, inc=1, device_id=where, device_id_type=MESH)

    units = chunks * 4

    def unit_of(u):
        chunk, step = u // 4, lax.rem(u, 4)
        far = 2 - 2 * (tp // 2) + lax.rem(core + step, 2)
        near = 2 * (tp // 2) + lax.rem(core + step + 1, 2)
        return chunk, step, jnp.where(step < 2, far, near)

    def fetch(u):
        chunk, step, dest = unit_of(u)
        start = dest * tile_cols + lax.rem(chunk, per_layer) * width
        slot = lax.rem(u, STAGES)
        return pltpu.make_async_copy(
            flat.at[chunk // per_layer, :, :, pl.ds(pl.multiple_of(start, LANES), width)],
            stage.at[slot], stage_sem.at[slot],
        )

    for u in range(STAGES):
        fetch(u).start()

    group = N_Y * each
    own = [
        pltpu.make_async_copy(
            probes.at[pl.ds((at * 2 + lo) * group, group)],
            features.at[z, y, pl.ds(lo * half + at * group, group)],
            own_p.at[at * 2 + lo],
        )
        for at in range(N_Z) for lo in range(2)
    ]
    for copy in own:
        copy.start()
    share = pl.ds(pl.multiple_of(core * half, half), half)
    along_y = pl.ds(pl.multiple_of(core * half, half // 2), half // 2)
    along_z = pl.ds(pl.multiple_of(core * half + half // 2, half // 2), half // 2)

    def share_own():
        for by in (2, 1, 3):
            _, where_y = peer(0, by)
            _, where_z = peer(by, 0)
            for rows_of, where in ((along_y, where_y), (along_z, where_z)):
                block = features.at[z, y, rows_of]
                remote(block, block, send_p, recv_p.at[0], where).start()

    def share_lines():
        drained(features.at[0, pl.ds(0, 3), share], recv_p.at[0])
        for by in (2, 1, 3):
            _, where_y = peer(0, by)
            _, where_z = peer(by, 0)
            for line, where in ((features.at[z, :, along_y], where_z), (features.at[:, y, along_z], where_y)):
                remote(line, line, send_p, recv_p.at[1], where).start()

    held = stage.shape[1]
    row = lax.broadcasted_iota(jnp.int32, (pair, 2 * held), 0)
    col = lax.broadcasted_iota(jnp.int32, (pair, 2 * held), 1)

    own_rows = pl.ds(pl.multiple_of(tp * rows, rows), rows)
    near_rows = pl.ds(pl.multiple_of((tp // 2) * pair, pair), pair)
    far_rows = pl.ds(pl.multiple_of((1 - tp // 2) * pair, pair), pair)

    def pick(u):
        chunk, step, dest = unit_of(u)
        slot = lax.rem(u, STAGES)
        fetch(u).wait()
        layer = chunk // per_layer
        wanted = jnp.where(row < rows, 2 * (row + offsets[layer, 0]), 2 * (row - rows + offsets[layer, 1]) + 1)
        chosen = jnp.where(col == wanted, 1.0, 0.0).astype(jnp.bfloat16)

        def picked(store):
            for at in range(0, blocks, 2):
                both = stage[slot, :, :, at * LANES:(at + 2) * LANES].reshape(2 * held, 2 * LANES)
                out = jnp.dot(chosen, both, preferred_element_type=jnp.float32).astype(jnp.bfloat16)
                for block in range(2):
                    for tensor in range(2):
                        store(at + block, tensor, out[
                            tensor * rows:(tensor + 1) * rows, block * LANES:(block + 1) * LANES
                        ])

        @pl.when(step < 3)
        def _():
            def store(block, tensor, value):
                to_tp[chunk, tensor, step, block] = value

            picked(store)

        @pl.when(step == 3)
        def _():
            def store(block, tensor, value):
                tile[chunk, block, tensor, own_rows] = value

            picked(store)

        @pl.when(u + STAGES < units)
        def _():
            fetch(u + STAGES).start()

    def ship(u, _):
        chunk, step, dest = unit_of(u)

        def send(recv):
            for tensor in range(2):
                remote(
                    to_tp.at[chunk, tensor, step], tile.at[chunk, :, tensor, own_rows],
                    send_a, recv.at[chunk], {"tp": dest},
                ).start()

        @pl.when(step < 2)
        def _():
            send(recv_a)

        @pl.when(step == 2)
        def _():
            send(recv_n)

        @pl.when(u + 1 < units)
        def _():
            pick(u + 1)

        return 0

    def spread(chunk, which):
        for dz, dy in STEPS:
            at, where = peer(dz, dy)
            remote(
                tile.at[chunk, at, :, which], column.at[chunk, mine, :, which],
                send_b, recv_b.at[chunk], where,
            ).start()

    def spread_near(chunk):
        drained(to_tp.at[0, :, 0], recv_n.at[chunk])
        spread(chunk, near_rows)

    def picks(chunk, _):
        lax.fori_loop(chunk * 4, chunk * 4 + 4, ship, 0)

        @pl.when(chunk > 0)
        def _():
            spread_near(chunk - 1)

        @pl.when(chunk == 2)
        def _():
            share_lines()

        return 0

    pick(0)
    for copy in own:
        copy.wait()
    pl.semaphore_wait(barrier, len(met))
    share_own()
    lax.fori_loop(0, chunks, picks, 0)
    spread_near(chunks - 1)

    drained(features.at[pl.ds(0, 3), :, share], recv_p.at[1])
    neighbour = {"tp": tp + 1 - 2 * core}

    def hand_on(step, _):
        at = lax.rem(mine + step + 1, N_Q)
        block = features.at[at // N_Y, lax.rem(at, N_Y), share]
        remote(block, block, send_f, recv_f, neighbour).start()
        return 0

    lax.fori_loop(0, N_Q - 1, hand_on, 0)
    others = column.at[0, pl.ds(0, N_Q - 1)]
    drained(others, recv_f)

    def spread_far(chunk):
        drained(to_tp.at[0, :, pl.ds(0, 2)], recv_a.at[chunk])
        spread(chunk, far_rows)
        column[chunk, mine] = tile[chunk, mine]

    keep = pl.ds(pl.multiple_of(x_lo * half, half), half)
    give = pl.ds(pl.multiple_of((1 - x_lo) * half, half), half)

    def multiply(chunk):
        drained(column.at[chunk, pl.ds(0, N_Q - 1)], recv_b.at[chunk])

        def product(turn, _):
            part = pl.ds(pl.multiple_of(lax.rem(1 - x_lo + turn, 2) * half, half), half)
            left = jnp.concatenate([features[at // N_Y, at % N_Y, part] for at in range(N_Q)], axis=1)
            right = jnp.concatenate([
                jnp.concatenate([column[chunk, at, 0], column[chunk, at, 1]], axis=1) for at in range(N_Q)
            ], axis=0)
            total[chunk, part] = jnp.dot(left, right, preferred_element_type=jnp.float32)

            @pl.when((turn == 0) & (chunk < chunks - 1))
            def _():
                remote(total.at[chunk, give], other.at[chunk], send_r, recv_r.at[chunk], partner).start()

            @pl.when((turn == 0) & (chunk == chunks - 1))
            def _():
                for dz, dy in STEPS + ((0, 0),):
                    at, where = peer(dz, dy)
                    remote(
                        total.at[chunk, rows_for(1 - x_lo, at)], ends.at[x_lo * N_Q + mine],
                        send_e, recv_e, {"grp": where["grp"] + 4 - 8 * x_lo},
                    ).start()

            @pl.when((turn == 1) & (chunk == chunks - 1))
            def _():
                for dz, dy in STEPS:
                    at, where = peer(dz, dy)
                    remote(
                        total.at[chunk, rows_for(x_lo, at)], ends.at[x_lo * N_Q + mine], send_e, recv_e, where,
                    ).start()

            return 0

        lax.fori_loop(0, 2, product, 0)

    def rows_for(lo, at):
        return pl.ds(pl.multiple_of(lo * half + at * each, each), each)

    def gate_of(sums):
        v, up = sums[..., :LANES], sums[..., LANES:]
        return (v / (1.0 + jnp.exp(-v)) * up).astype(jnp.bfloat16)

    def gate(chunk):
        drained(other.at[chunk], recv_r.at[chunk])
        gated[chunk] = gate_of(total[chunk, keep] + other[chunk]).reshape(N_Q, each, LANES)
        check[mine, chunk] = gated[chunk, mine]
        for dz, dy in STEPS:
            at, where = peer(dz, dy)
            remote(gated.at[chunk, at], check.at[mine, chunk], send_h, recv_h, where).start()

    def step(chunk, _):
        spread_far(chunk)

        @pl.when(chunk >= LAG)
        def _():
            multiply(chunk - LAG)

        return 0

    def finish(chunk, _):
        multiply(chunk)
        gate(chunk - LAG)
        return 0

    lax.fori_loop(0, chunks, step, 0)
    lax.fori_loop(chunks - LAG, chunks, finish, 0)
    for chunk in range(chunks - LAG, chunks - 1):
        gate(chunk)
    ends[x_lo * N_Q + mine] = total[chunks - 1, rows_for(x_lo, mine)]
    came = ends.at[pl.ds(0, 2 * N_Q - 1)]
    drained(came, recv_e)
    last = gate_of(ends[:N_Q] + ends[N_Q:])
    for at in range(N_Q):
        check[at, chunks - 1] = last[at]

    arrived = check.at[pl.ds(0, N_Q - 1), pl.ds(0, chunks - 1)]
    drained(arrived, recv_h)
    drained(to_tp, send_a)
    drained(column.at[:, pl.ds(0, N_Q - 1)], send_b)
    for sem in (send_p, send_f):
        drained(others, sem)
    drained(other.at[pl.ds(0, chunks - 1)], send_r)
    drained(came, send_e)
    drained(arrived, send_h)


def place(tile, check, tiles_out, check_out, lines, sem, line_sem):
    chunks, blocks = tile.shape[:2]
    layers = tiles_out.shape[0]
    per_layer = chunks // layers
    for chunk in range(chunks):
        for block in range(blocks):
            start = (chunk % per_layer * blocks + block) * LANES
            lines[chunk // per_layer, :, start:start + LANES] = check[block, chunk]
    small = pltpu.make_async_copy(lines, check_out, line_sem)
    small.start()
    for chunk in range(chunks):
        for block in range(blocks):
            start = (chunk % per_layer * blocks + block) * LANES
            for tensor in range(2):
                copy = pltpu.make_async_copy(
                    tile.at[chunk, block, tensor],
                    tiles_out.at[chunk // per_layer, tensor, :, pl.ds(start, LANES)],
                    sem,
                )
                copy.start()
    small.wait()
    pltpu.make_async_copy(tile, tile, sem).wait()


def per_device(flat_shards, offsets, probes):
    tp_count = lax.axis_size("tp")
    layers = flat_shards.shape[0]
    rows = flat_shards.shape[2] - PAD
    tile_cols = flat_shards.shape[3] // tp_count
    tile_rows = rows * tp_count
    count = probes.shape[0]
    half = count // 2
    each = half // N_Q
    width = N_Q * LANES
    chunks = layers * (tile_cols // width)
    bf16, f32 = jnp.bfloat16, jnp.float32
    dma = pltpu.SemaphoreType.DMA
    tile, check = pl.pallas_call(
        functools.partial(kernel, layers),
        out_shape=(
            pltpu.VMEM((chunks, N_Q, 2, tile_rows, LANES), bf16),
            pltpu.VMEM((N_Q, chunks, each, LANES), bf16),
        ),
        in_specs=[
            pl.BlockSpec(memory_space=pl.ANY),
            pl.BlockSpec(memory_space=pltpu.SMEM),
            pl.BlockSpec(memory_space=pl.ANY),
        ],
        out_specs=(pl.BlockSpec(memory_space=pltpu.VMEM), pl.BlockSpec(memory_space=pltpu.VMEM)),
        scratch_shapes=[
            pltpu.VMEM((STAGES, rows + PAD, 2, width), bf16),
            pltpu.VMEM((chunks, 2, 3, N_Q, rows, LANES), bf16),
            pltpu.VMEM((chunks, N_Q, 2, tile_rows, LANES), bf16),
            pltpu.VMEM((N_Z, N_Y, count, probes.shape[1]), bf16),
            pltpu.VMEM((chunks, count, 2 * LANES), f32),
            pltpu.VMEM((chunks, half, 2 * LANES), f32),
            pltpu.VMEM((chunks, N_Q, each, LANES), bf16),
            pltpu.VMEM((2 * N_Q, each, 2 * LANES), f32),
            dma((STAGES,)), dma, dma((chunks,)), dma((chunks,)), dma, dma((chunks,)),
            dma((2 * N_Z,)), dma, dma((2,)), dma, dma,
            dma, dma((chunks,)), dma, dma, dma, dma,
        ],
        compiler_params=pltpu.CompilerParams(
            collective_id=0, has_side_effects=True, vmem_limit_bytes=51 * 2**20
        ),
        name="reshard_check",
    )(jnp.transpose(flat_shards, (0, 2, 1, 3)), offsets, probes)
    return pl.pallas_call(
        place,
        out_shape=(
            jax.ShapeDtypeStruct((layers, 2, tile_rows, tile_cols), bf16),
            jax.ShapeDtypeStruct((layers, each, tile_cols), bf16),
        ),
        in_specs=[pl.BlockSpec(memory_space=pltpu.VMEM), pl.BlockSpec(memory_space=pltpu.VMEM)],
        out_specs=(pl.BlockSpec(memory_space=pl.ANY), pl.BlockSpec(memory_space=pl.ANY)),
        scratch_shapes=[pltpu.VMEM((layers, each, tile_cols), bf16), dma, dma],
        compiler_params=pltpu.CompilerParams(vmem_limit_bytes=16 * 2**20),
        name="place",
    )(tile, check)


def solution(mesh):
    placed = (P(None, None, ("grp", "tp"), None), P(), P(None, "grp"))
    return jax.shard_map(
        per_device,
        mesh=mesh,
        in_specs=placed,
        out_specs=(P(None, None, "grp", "tp"), P(None, "grp", "tp")),
        check_vma=False,
    )
```
